32 devices in a mesh: row: 8 (over z, x), col: 4 (over y, core).
Axes of the slice: x: 2, y: 2, z: 4, core: 2. Of those that a mesh axis runs over, the one named last changes fastest.
Arguments:
- gradient: bfloat16 [3072, 14336], P('row', 'col'), may hold values from -0.1875 to 0.1875
- left_factor: float32 [3072, 3072], P('row', 'col'), may hold values from -1 to 11, as said below
- right_factor: float32 [14336, 14336], P('col', 'row'), may hold values from -1 to 3, as said below
- left_basis: bfloat16 [3072, 3072], P('row', 'col'), may hold values from -0.109375 to 0.109375
- right_basis: bfloat16 [14336, 2048], P('row', 'col'), may hold values from -0.046875 to 0.046875
Outputs:
- left_new: float32 [3072, 3072], P('row', 'col')
- right_new: float32 [14336, 14336], P('col', 'row')
- left_out: float32 [3072, 3072], P('row', 'col')
- right_out: float32 [14336, 2048], P('col', 'row')
The draws below stay inside these ranges and needn't reach their ends.
Inputs may be any that keep to these rules, and one draw needn't show every extreme that they name: left_factor is symmetric. right_factor is symmetric.
All inputs are finite; a program needn't handle non-finite values.
Results may differ from the reference program's by a relative error of at most 0.0029.
Values may be sent and summed in bfloat16 or wider, within the bound.
A program may use at most 192 MiB of HBM per device.

```python
import math
import jax
import jax.numpy as jnp
from jax import lax

DMODEL = 3072
DHIDDEN = 14336
NVEC = 2048


def factor_draw(key, size, level):
    noise = jax.random.truncated_normal(jax.random.fold_in(key, 11), -4.0, 4.0, (size, size), jnp.float32)
    noise = noise * (0.4 / math.sqrt(size))
    symmetric = noise + noise.T
    place = jnp.arange(size, dtype=jnp.float32) / size
    spread = jax.random.uniform(jax.random.fold_in(key, 12), (size,), jnp.float32, -1.2, 1.2)
    scaling = jnp.sqrt(level * jnp.exp(math.log(3.0) * place + spread))
    base = jnp.eye(size, dtype=jnp.float32) + symmetric
    return scaling[:, None] * base * scaling[None, :]


def draw_left_factor(key, part):
    return factor_draw(jax.random.fold_in(key, 21), DMODEL, 1.0)


def draw_right_factor(key, part):
    return factor_draw(jax.random.fold_in(key, 22), DHIDDEN, DMODEL / DHIDDEN)


def steps_of(own_key, shape, shards, least, top_value):
    loudness, own = 1.0, jax.random.fold_in(own_key, 6)
    for position, shards_of in shards:
        heights = jnp.exp(jax.random.uniform(jax.random.fold_in(own, position), (shards_of,), jnp.float32, least / len(shards), top_value / len(shards)))
        loudness = loudness * jnp.repeat(heights, shape[position] // shards_of).reshape([-1 if axis == position else 1 for axis in range(len(shape))])
    return loudness


def scatter_about(stream_key, extent, scale, limit, pieces=(), held_as=jnp.bfloat16):
    array = jax.random.normal(stream_key, extent, jnp.float32) * scale
    if len(pieces) > 0:
        array = steps_of(stream_key, extent, pieces, -0.22, 0.18) * array
    return jnp.clip(array, min=-limit, max=limit).astype(held_as)


def setup_inputs(seed: int = 0) -> dict:
    streams_of = jax.random.split(jax.random.key(seed), 6)
    return {
        "gradient": scatter_about(streams_of[0], (DMODEL, DHIDDEN), (DHIDDEN // 16) ** -0.5, 0.1875, ((0, 8), (1, 4))),
        "left_factor": draw_left_factor(jax.random.fold_in(streams_of[5], 71), 0),
        "right_factor": draw_right_factor(jax.random.fold_in(streams_of[5], 71), 0),
        "left_basis": scatter_about(streams_of[3], (DMODEL, DMODEL), DMODEL ** -0.5, 0.109375, ((0, 8), (1, 4))),
        "right_basis": scatter_about(streams_of[4], (DHIDDEN, NVEC), DHIDDEN ** -0.5, 0.046875, ((0, 8), (1, 4))),
    }


ema_decay = 0.95
epsilon = 1e-06

def reference(gradient, left_factor, right_factor, left_basis, right_basis):
    gram_left = lax.dot_general(gradient, gradient, (((1,), (1,)), ((), ())), preferred_element_type=jnp.float32)
    gram_right = lax.dot_general(gradient, gradient, (((0,), (0,)), ((), ())), preferred_element_type=jnp.float32)
    left_new = ema_decay * left_factor + (1.0 - ema_decay) * gram_left
    right_new = ema_decay * right_factor + (1.0 - ema_decay) * gram_right
    left_half = left_new.astype(jnp.bfloat16)
    right_half = right_new.astype(jnp.bfloat16)
    left_prod = jnp.dot(left_half, left_basis, preferred_element_type=jnp.float32)
    right_prod = jnp.dot(right_half, right_basis, preferred_element_type=jnp.float32)
    left_sq = lax.optimization_barrier(jnp.sum(left_prod * left_prod, axis=0))
    right_sq = lax.optimization_barrier(jnp.sum(right_prod * right_prod, axis=0))
    left_out = left_prod * lax.rsqrt(left_sq / DMODEL + epsilon)
    right_out = right_prod * lax.rsqrt(right_sq / DHIDDEN + epsilon)
    return (left_new, right_new, left_out, right_out)
```

```python
import jax
import jax.numpy as jnp
from jax import lax
from jax.sharding import PartitionSpec as P

ema_decay = 0.95
epsilon = 1e-06


def dot(a, b, dims):
    return lax.dot_general(a, b, (dims, ((), ())), preferred_element_type=jnp.float32)


def make_body(row_count, col_count, dmodel, dhidden):
    ring = list(range(0, row_count, 2)) + list(range(1, row_count, 2))[::-1]
    place = [ring.index(r) for r in range(row_count)]
    forward = [(ring[i], ring[(i + 1) % row_count]) for i in range(row_count)]
    backward = [(b, a) for a, b in forward]
    group_ratio = row_count // col_count
    pair_count = row_count // 2

    def flat(r, c):
        return r * col_count + c

    def spread(block):
        row, col = lax.axis_index("row"), lax.axis_index("col")
        owner = row // group_ratio
        result = block
        for step in range(1, col_count // 2):
            perm = []
            for r in range(row_count):
                o = r // group_ratio
                perm.append((flat(r, o), flat(r, (o + 2 * step) % col_count)))
            got = lax.ppermute(block, ("row", "col"), perm)
            result = jnp.where(col == (owner + 2 * step) % col_count, got, result)
        perm = []
        for r in range(row_count):
            o = r // group_ratio
            perm += [(flat(r, c), flat(r, c ^ 1)) for c in range(col_count) if (c - o) % 2 == 0]
        got = lax.ppermute(result, ("row", "col"), perm)
        return jnp.where((col - owner) % 2 == 0, result, got)

    def on_device(gradient, left_factor, right_factor, left_basis, right_basis):
        row = lax.axis_index("row")
        rows, cols = gradient.shape
        half = rows // 2
        slab_cols = cols // group_ratio
        first_col = row % group_ratio * slab_cols
        my_place = jnp.asarray(place)[row]
        members = jnp.asarray(ring)

        basis_full = lax.all_gather(right_basis, "col", axis=1, tiled=True)
        left_basis_cols = lax.all_gather(left_basis, "row", axis=0, tiled=True)

        right_new = ema_decay * right_factor
        gram_part = jnp.zeros((dmodel, rows), jnp.float32)

        ups, downs = gradient[:half], gradient[half:]
        batch = [ups, downs]
        origins = [(row * rows), (row * rows + half)]
        cuts = sorted({row_count - 1, max(row_count - 3, 0), (row_count - 1) // 2})
        for step in range(row_count):
            if step > 0:
                ups = lax.ppermute(ups, "row", forward)
                downs = lax.ppermute(downs, "row", backward)
                batch += [ups, downs]
                origins += [
                    members[(my_place - step) % row_count] * rows,
                    members[(my_place + step) % row_count] * rows + half,
                ]
            if step in cuts:
                piece = jnp.concatenate(batch, axis=0)
                offered = lax.dynamic_slice_in_dim(piece, first_col, slab_cols, 1)
                shared = spread(offered)
                right_new = right_new + (1.0 - ema_decay) * dot(piece, shared, ((0,), (0,)))
                left = dot(piece, gradient, ((1,), (1,)))
                for n, origin in enumerate(origins):
                    gram_part = lax.dynamic_update_slice_in_dim(
                        gram_part, left[n * half : (n + 1) * half], origin, 0
                    )
                batch, origins = [], []

        gram_block = lax.psum_scatter(gram_part, "col", scatter_dimension=0, tiled=True).T
        left_new = ema_decay * left_factor + (1.0 - ema_decay) * gram_block
        left_rows = lax.all_gather(left_new.astype(jnp.bfloat16), "col", axis=1, tiled=True)
        left_prod = dot(left_rows, left_basis_cols, ((1,), (0,)))

        right_half = right_new.astype(jnp.bfloat16)
        nvec = basis_full.shape[1]
        width = nvec // row_count
        by_dest = basis_full.reshape(-1, pair_count, 2, width)
        even = by_dest[:, :, 0].reshape(-1, pair_count * width)
        odd = by_dest[:, :, 1].reshape(-1, pair_count * width)
        mine_even = row % 2 == 0
        basis_keep = jnp.where(mine_even, even, odd)
        basis_send = jnp.where(mine_even, odd, even)
        pair = row // 2
        swap = [(r, r ^ 1) for r in range(row_count)]
        chunks = 4
        depth = right_half.shape[0] // chunks
        parts = []
        for n in range(chunks):
            block = right_half[n * depth : (n + 1) * depth]
            away = dot(block, basis_send, ((1,), (0,))).astype(jnp.bfloat16)
            got = lax.ppermute(away, "row", swap)
            total = dot(block, basis_keep, ((1,), (0,))) + got.astype(jnp.float32)
            own = lax.dynamic_slice_in_dim(total, pair * width, width, 1)
            for d in range(1, pair_count):
                perm = [(r, (r + 2 * d) % row_count) for r in range(row_count)]
                there = (pair + d) % pair_count
                out = lax.dynamic_slice_in_dim(total, there * width, width, 1)
                own = own + lax.ppermute(out.astype(jnp.bfloat16), "row", perm).astype(jnp.float32)
            parts.append(own)
        right_prod = jnp.concatenate(parts, axis=0)

        left_sq = lax.psum(jnp.sum(left_prod * left_prod, axis=0), "row")
        left_out = left_prod * lax.rsqrt(left_sq / dmodel + epsilon)
        right_sq = lax.psum(jnp.sum(right_prod * right_prod, axis=0), "col")
        right_out = right_prod * lax.rsqrt(right_sq / dhidden + epsilon)
        return (left_new, right_new, left_out, right_out)

    return on_device


def solution(mesh):
    in_specs = (P("row", "col"), P("row", "col"), P("col", "row"), P("row", "col"), P("row", "col"))
    out_specs = (P("row", "col"), P("col", "row"), P("row", "col"), P("col", "row"))

    def step(gradient, left_factor, right_factor, left_basis, right_basis):
        dmodel, dhidden = gradient.shape
        body = make_body(mesh.shape["row"], mesh.shape["col"], dmodel, dhidden)
        return jax.shard_map(
            body, mesh=mesh, in_specs=in_specs, out_specs=out_specs, check_vma=False
        )(gradient, left_factor, right_factor, left_basis, right_basis)

    return step
```
